32 devices in a mesh: row: 8 (over z, core), col: 4 (over y, x).
Axes of the slice: x: 2, y: 2, z: 4, core: 2. Of those that a mesh axis runs over, the one named last changes fastest.
Arguments:
- pair_exchange: bfloat16 [64, 16, 1024], P(('row', 'col')), may hold values from -6 to 6
- conduction: bfloat16 [64, 4, 1024], P(('row', 'col')), may hold values from -6 to 6
- valence: bfloat16 [64, 4, 1024], P(('row', 'col')), may hold values from -6 to 6
- coulomb: float32 [1024], replicated, may hold values from 0.5 to 5
- screening: float32 [34, 1024], replicated, may hold values from 0.1 to 1
- energies: float32 [64, 16], P(('row', 'col')), may hold values from 1 to 9
- vectors: bfloat16 [64, 512], P(('row', 'col')), may hold values from -6 to 6
- k_coords: int32 [64, 2], P(('row', 'col')), may hold values from 0 to 31, as said below
Outputs:
- residual_block: float32 [64, 512], P(('row', 'col'))
- alpha: float32 [32, 32], replicated
The draws below stay inside these ranges and needn't reach their ends.
Inputs may be any that keep to these rules, and one draw needn't show every extreme that they name: `k_coords`: each row holds a k-point's coordinates on the periodic 32 x 2 mesh, first then second; every mesh point occurs exactly once.
All inputs are finite; a program needn't handle non-finite values.
Results may differ from the reference program's by a relative error of at most 0.0028.
Values may be sent and summed in bfloat16 or wider, within the bound.
A program may use at most 64 MiB of HBM per device.

```python
import math
import jax
import jax.numpy as jnp
from jax import lax

NV = 4
NC = 4
NB = 16
NG = 1024
NVEC = 32
MX = 32
NK = 64
MY = 2
NT = 1024
NQF = 34


def draw_energies(key, part):
    ramp = 1.0 + 2.0 * jnp.arange(NK, dtype=jnp.float32)[:, None] / NK
    base = jnp.exp(jax.random.uniform(key, (NK, NB), jnp.float32, 0.0, math.log(3.0)))
    return (base * ramp).astype(jnp.float32)


def draw_k_coords(key, part):
    order = jax.random.permutation(key, NK)
    return jnp.stack([order // MY, order % MY], axis=1).astype(jnp.int32)


def block_levels(key, dims, shards, least, largest):
    level = 1.0
    for axis_at, blocks in shards:
        draws = jax.random.uniform(jax.random.fold_in(jax.random.fold_in(key, 6), axis_at), (blocks,), jnp.float32, least / len(shards), largest / len(shards))
        level = level * jnp.repeat(jnp.exp(draws), dims[axis_at] // blocks).reshape((-1,) + (1,) * (len(dims) - 1 - axis_at))
    return level


def bell_draw(own_key, extent, spread, limit, cuts=(), kind=jnp.bfloat16):
    factor_of = block_levels(own_key, extent, cuts, -0.22, 0.18) if cuts else 1.0
    values = jax.random.normal(own_key, extent, jnp.float32) * spread * factor_of
    return jnp.minimum(jnp.maximum(values, -limit), limit).astype(kind)


def setup_inputs(seed: int = 0) -> dict:
    key_of = jax.random.split(jax.random.key(seed), 9)
    pair_exchange = bell_draw(key_of[0], (NK, NB, NG), 1.0, 6.0, ((0, 32),))
    conduction = bell_draw(key_of[1], (NK, NC, NG), 1.0, 6.0, ((0, 32),))
    valence = bell_draw(key_of[2], (NK, NV, NG), 1.0, 6.0, ((0, 32),))
    coulomb = jnp.clip(jnp.exp(jax.random.uniform(key_of[3], (NG,), jnp.float32, math.log(0.5), math.log(5.0))), 0.5, 5.0)
    screening = jnp.clip(jnp.exp(jax.random.uniform(key_of[4], (NQF, NG), jnp.float32, math.log(0.1), math.log(1.0))), 0.1, 1.0)
    energies = draw_energies(jax.random.fold_in(key_of[8], 71), 0)
    vectors = bell_draw(key_of[6], (NK, NB * NVEC), 1.0, 6.0, ((0, 32),))
    k_coords = draw_k_coords(jax.random.fold_in(key_of[8], 71), 0)
    return dict(pair_exchange=pair_exchange, conduction=conduction, valence=valence, coulomb=coulomb, screening=screening, energies=energies, vectors=vectors, k_coords=k_coords)


highest = lax.Precision.HIGHEST


def reference(pair_exchange, conduction, valence, coulomb, screening, energies, vectors, k_coords):
    moving = vectors.astype(jnp.float32).reshape(NK, NB, NVEC)
    joined = (valence.astype(jnp.float32)[:, :, None, :] * conduction.astype(jnp.float32)[:, None, :, :]).reshape(NK, NB, NG)
    pair_rows = lax.optimization_barrier(joined.astype(jnp.bfloat16)).astype(jnp.float32)
    along_first = jnp.arange(MX)
    along_second = jnp.arange(MY)
    fold_first = jnp.minimum(along_first, MX - along_first)
    fold_second = jnp.minimum(along_second, MY - along_second)
    mesh_index = (fold_first[:, None] * (MY // 2 + 1) + fold_second[None, :]).astype(jnp.int32)
    spectrum = jnp.fft.fft2(screening[mesh_index], axes=(0, 1)).real
    density = jnp.einsum("ktg,ktn->gn", pair_exchange.astype(jnp.float32), moving, precision=highest)
    place_first = k_coords[:, 0]
    place_second = k_coords[:, 1]
    block_size = 64 if NG % 64 == 0 else NG

    def one_block(running, anchor):
        piece_rows = lax.dynamic_slice_in_dim(pair_rows, anchor, block_size, 2)
        projected = jnp.einsum("ktg,ktn->kgn", piece_rows, moving, precision=highest)
        mesh_grid = jnp.zeros((MX, MY, block_size, NVEC), jnp.float32).at[place_first, place_second].set(projected)
        spectrum_part = lax.dynamic_slice_in_dim(spectrum, anchor, block_size, 2)
        potential = jnp.fft.ifft2(jnp.fft.fft2(mesh_grid, axes=(0, 1)) * spectrum_part[:, :, :, None], axes=(0, 1)).real
        sampled = potential[place_first, place_second]
        return running + jnp.einsum("ktg,kgn->ktn", piece_rows, sampled, precision=highest), None

    anchors = (jnp.arange(NG // block_size) * block_size).astype(jnp.int32)
    direct, _ = lax.scan(one_block, jnp.zeros((NK, NB, NVEC), jnp.float32), anchors)
    exchange_term = jnp.einsum("ktg,gn->ktn", pair_exchange.astype(jnp.float32) * coulomb, density, precision=highest)
    applied = energies[:, :, None] * moving + (2.0 / NT) * exchange_term - direct / NK
    alpha = jnp.einsum("ktm,ktn->mn", moving, applied, precision=highest) / NT
    residual = applied - jnp.einsum("ktm,mn->ktn", moving, alpha, precision=highest)
    return residual.reshape(NK, NB * NVEC), alpha
```

```python
import functools

import jax
import jax.numpy as jnp
from jax import lax
from jax.experimental import pallas as pl
from jax.experimental.pallas import tpu as pltpu
from jax.sharding import PartitionSpec as P

MX = 32
LANES = 128
MESH = pl.DeviceIdType.MESH
F32 = jnp.float32
BF16 = jnp.bfloat16


def split_pair(value):
    high = value.astype(BF16)
    return high, (value - high.astype(F32)).astype(BF16)


def dot(a, b, contract):
    return lax.dot_general(a, b, ((contract[0:1], contract[1:2]), ((), ())), preferred_element_type=F32)


def iota(shape, axis):
    return lax.broadcasted_iota(jnp.int32, shape, axis)


def one_hot(condition):
    return jnp.where(condition, 1.0, 0.0).astype(BF16)


def kernel(
    dims, msg_ref, px_ref, wide_ref, coulomb_ref, screening_ref,
    out_ref, alpha_ref,
    slots, px_slots, sel_v, sel_c, tile_m, block_m, perm, sel_k, screen, tiled, pairs, proj, coords, coupling,
    dens_slots, partial, out_send, out_slots, gram_slots,
    in_send, in_recv, px_send, px_recv, dens_send, dens_recv, gram_send, gram_recv, o_send, o_recv,
):
    rows, cols, nk, nv, nc, nvec, total, mesh_cols = dims
    row, col = lax.axis_index("row"), lax.axis_index("col")
    me = row * cols + col
    count = rows * cols
    kb = rows * nk
    nb = nv * nc
    unit = nk * nv
    per = kb * nv
    batch = per * nc

    def other(step):
        peer = lax.rem(me + step, count)
        return peer // cols, lax.rem(peer, cols)

    barrier = pltpu.get_barrier_semaphore()

    def greet(step, carry):
        pr, pc = other(step)
        pl.semaphore_signal(barrier, inc=1, device_id=(pr, pc), device_id_type=MESH)
        return carry

    lax.fori_loop(1, count, greet, 0)

    at = iota((batch, rows * 16), 0)
    to = iota((batch, rows * 16), 1)
    base = (at // unit) % rows * 16 + (at // nv) % nk * 8
    sel_v[...] = one_hot(to == base + at % nv)
    sel_c[...] = one_hot(to == base + nv + at // per)
    at = iota((LANES, nc * LANES), 0)
    to = iota((LANES, nc * LANES), 1)
    tile_m[...] = one_hot((at // nvec == to // LANES) & (at % nvec == to % nvec))
    at = iota((batch, kb * nvec), 0)
    to = iota((batch, kb * nvec), 1)
    block_m[...] = one_hot((at // nv) % kb == to // nvec)
    at = iota((batch, rows * nk * nb), 0)
    to = iota((batch, rows * nk * nb), 1)
    perm[...] = one_hot(to == (at // nv) % kb * nb + at % nv * nc + at // per)
    at = iota((2 * cols * kb, count * 8), 0)
    to = iota((2 * cols * kb, count * 8), 1)
    point = at % (cols * kb)
    sel_k[...] = one_hot(to == point // nk * 8 + at // (cols * kb) * nk + point % nk)
    screen[...] = jnp.zeros_like(screen)
    mine = pl.ds(pl.multiple_of(row * LANES, LANES), LANES)
    high, low = split_pair(jnp.concatenate(
        [screening_ref[:, mine], jnp.zeros((LANES - screening_ref.shape[0], LANES), F32)], axis=0))
    screen[0:LANES] = high
    screen[LANES:2 * LANES] = low

    pl.semaphore_wait(barrier, count - 1)

    def in_copy(step):
        pr, pc = other(step)
        return pltpu.make_async_remote_copy(
            src_ref=msg_ref.at[pr], dst_ref=slots.at[col, row],
            send_sem=in_send.at[pc, pr], recv_sem=in_recv.at[col, row],
            device_id=(pr, pc), device_id_type=MESH)

    def px_copy(step):
        pr = lax.rem(row + step, rows)
        return pltpu.make_async_remote_copy(
            src_ref=px_ref.at[:, :, pl.ds(pl.multiple_of(pr * LANES, LANES), LANES)], dst_ref=px_slots.at[row],
            send_sem=px_send.at[pr], recv_sem=px_recv.at[row],
            device_id=(pr, col), device_id_type=MESH)

    def dens_copy(step):
        pc = lax.rem(col + step, cols)
        return pltpu.make_async_remote_copy(
            src_ref=dens_slots.at[col], dst_ref=dens_slots.at[col],
            send_sem=dens_send.at[pc], recv_sem=dens_recv.at[col],
            device_id=(row, pc), device_id_type=MESH)

    def gram_copy(step):
        pr, pc = other(step)
        return pltpu.make_async_remote_copy(
            src_ref=gram_slots.at[me], dst_ref=gram_slots.at[me],
            send_sem=gram_send.at[pr * cols + pc], recv_sem=gram_recv.at[me],
            device_id=(pr, pc), device_id_type=MESH)

    def o_copy(step):
        pr = lax.rem(row + step, rows)
        return pltpu.make_async_remote_copy(
            src_ref=out_send.at[pr], dst_ref=out_slots.at[row],
            send_sem=o_send.at[pr], recv_sem=o_recv.at[row],
            device_id=(pr, col), device_id_type=MESH)

    def start_all(copy, end):
        def body(step, carry):
            copy(step).start()
            return carry
        lax.fori_loop(1, end, body, 0)

    def landed(ref, sem):
        pltpu.make_async_copy(ref, ref, sem).wait()

    start_all(px_copy, rows)
    start_all(in_copy, count)
    slots[col, row] = msg_ref[row]
    px_slots[row] = px_ref[:, :, mine]

    def take_batch(which):
        def wait_one(r, carry):
            @pl.when((r != row) | (which != col))
            def _():
                landed(slots.at[which, r], in_recv.at[which, r])
            return carry
        lax.fori_loop(0, rows, wait_one, 0)
        got = slots[which]
        factors = got[:, 0:16, :].reshape(rows * 16, LANES)
        rest = got[:, 16:32, :].astype(F32)
        packed = rest[:, 0:8, :].reshape(per, LANES).astype(BF16)
        coords[which] = rest[:, 8:16, :].reshape(rows * 8, LANES).astype(BF16)
        wide = dot(packed, tile_m[...], (1, 0)).astype(BF16)
        stacked = jnp.concatenate([wide[:, s * LANES:(s + 1) * LANES] for s in range(nc)], axis=0)
        tiled[which] = stacked
        joined = (dot(sel_v[...], factors, (1, 0)) * dot(sel_c[...], factors, (1, 0))).astype(BF16)
        pairs[which] = joined.astype(F32)
        spread = jnp.concatenate([stacked] * (kb * nvec // LANES), axis=1) * block_m[...]
        projected = dot(spread, joined, (0, 0))
        proj[pl.ds(which * kb, kb)] = projected.reshape(kb, nvec, LANES)

    take_batch(col)

    def px_wait(step, carry):
        r = lax.rem(row + step, rows)
        landed(px_slots.at[r], px_recv.at[r])
        return carry

    lax.fori_loop(1, rows, px_wait, 0)
    px = dot(perm[...], px_slots[...].reshape(rows * nk * nb, LANES), (1, 0)).astype(BF16)
    own_x = tiled[col][:, 0:nvec]
    dens_slots[col] = dot(own_x, px, (0, 0))
    start_all(dens_copy, cols)

    def rest_batches(step, carry):
        take_batch(lax.rem(col + step, cols))
        return carry

    lax.fori_loop(1, cols, rest_batches, 0)

    place = dot(sel_k[...], coords[...].reshape(count * 8, LANES), (1, 0))
    points = cols * kb
    first, second = place[0:points], place[points:2 * points]
    lane = iota((points, LANES), 1).astype(F32)
    coupling[0, 0:points] = first
    coupling[1, 0:points] = second
    start = pl.multiple_of(col * kb, kb)
    own_first = coupling[0, pl.ds(start, kb), :]
    own_second = coupling[1, pl.ds(start, kb), :]
    hots = []
    for i in range(kb):
        da = jnp.abs(own_first[i:i + 1] - first)
        db = jnp.abs(own_second[i:i + 1] - second)
        q = jnp.minimum(da, MX - da) * (mesh_cols // 2 + 1) + jnp.minimum(db, mesh_cols - db)
        hots.append(one_hot(q == lane))
    for i in range(kb):
        coupling[i] = dot(jnp.concatenate([hots[i], hots[i]], axis=1), screen[...], (1, 0))

    def dens_wait(step, carry):
        c = lax.rem(col + step, cols)
        landed(dens_slots.at[c], dens_recv.at[c])
        return carry

    lax.fori_loop(1, cols, dens_wait, 0)
    density = dens_slots[0]
    for c in range(1, cols):
        density = density + dens_slots[c]
    high, low = split_pair(density * coulomb_ref[:, mine] * (2.0 / (total * nb)))
    partial[...] = (dot(px, high, (1, 1)) + dot(px, low, (1, 1))).reshape(nc, rows, unit, nvec)

    wide_own = wide_ref[...] * msg_ref[row, 16:32, :].astype(F32)[0:8]
    for s in range(nc):
        partial[s, row] = partial[s, row] + wide_own[:, s * nvec:(s + 1) * nvec]

    group = 4
    row_k = (iota((nc * unit, LANES), 0) // nv) % nk
    potentials = []
    for block in range(kb // group):
        def gather(j, sums):
            term = proj[j]
            return tuple(
                sums[u] + coupling[block * group + u, pl.ds(j, 1), :] * term for u in range(group))
        potentials += list(lax.fori_loop(
            0, points, gather, tuple(jnp.zeros((nvec, LANES), F32) for _ in range(group)), unroll=8))
    for r in range(rows):
        mine_pairs = pairs[col].reshape(nc, rows, unit, LANES)[:, r].reshape(nc * unit, LANES)
        left = jnp.concatenate(
            [jnp.where(row_k == k, mine_pairs, 0.0) for k in range(nk)], axis=1).astype(BF16)
        high, low = split_pair(jnp.concatenate([potentials[r * nk + k] for k in range(nk)], axis=1))
        direct = dot(left, high, (1, 1)) + dot(left, low, (1, 1))
        for s in range(nc):
            partial[s, r] = partial[s, r] - direct[s * unit:(s + 1) * unit] * (1.0 / total)

    whole = partial[...]
    packed = jnp.concatenate([whole[s].reshape(per, nvec) for s in range(nc)], axis=1)
    out_send[...] = packed.reshape(rows, unit, LANES)
    start_all(o_copy, rows)
    high, low = split_pair(whole.reshape(batch, nvec))
    gram = dot(own_x, high, (0, 0)) + dot(own_x, low, (0, 0))
    step = nvec // nc
    gram_slots[me] = jnp.concatenate([gram[s * step:(s + 1) * step] for s in range(nc)], axis=1)
    start_all(gram_copy, count)

    def o_wait(d, acc):
        r = lax.rem(row + d, rows)
        landed(out_slots.at[r], o_recv.at[r])
        return acc + out_slots[r]

    applied = lax.fori_loop(1, rows, o_wait, out_send[row])

    def gram_wait(d, carry):
        p = lax.rem(me + d, count)
        landed(gram_slots.at[p], gram_recv.at[p])
        return carry

    lax.fori_loop(1, count, gram_wait, 0)
    sums = jnp.sum(gram_slots[...], axis=0) * (1.0 / (total * nb))
    alpha = jnp.concatenate([sums[:, s * nvec:(s + 1) * nvec] for s in range(nc)], axis=0)
    alpha_ref[...] = alpha
    own = msg_ref[row, 16:32, :].astype(F32)[0:8]
    own_rows = jnp.concatenate([own[:, s * nvec:(s + 1) * nvec] for s in range(nc)], axis=0).astype(BF16)
    high, low = split_pair(alpha)
    taken = dot(own_rows, high, (1, 0)) + dot(own_rows, low, (1, 0))
    residual = applied - jnp.concatenate([taken[s * unit:(s + 1) * unit] for s in range(nc)], axis=1)
    for j in range(nv):
        out_ref[:, j * LANES:(j + 1) * LANES] = jnp.concatenate(
            [residual[k * nv + j:k * nv + j + 1] for k in range(nk)], axis=0)

    def drain(copy, end):
        def body(d, carry):
            copy(d).wait_send()
            return carry
        lax.fori_loop(1, end, body, 0)

    drain(in_copy, count)
    drain(px_copy, rows)
    drain(dens_copy, cols)
    drain(o_copy, rows)
    drain(gram_copy, count)


def fast_on_device(pair_exchange, conduction, valence, coulomb, screening, energies, vectors, k_coords):
    nk, nb, planes = pair_exchange.shape
    nv, nc = valence.shape[1], conduction.shape[1]
    nvec = vectors.shape[1] // nb
    rows, cols = lax.axis_size("row"), lax.axis_size("col")
    count = rows * cols
    total = nk * count
    unit = nk * nv
    kb = rows * nk
    batch = kb * nb
    factors = jnp.concatenate([valence, conduction], axis=1).reshape(nk * (nv + nc), rows, LANES)
    packed = vectors.reshape(unit, LANES)
    spots = jnp.broadcast_to(k_coords.T.astype(BF16).reshape(2 * nk, 1), (2 * nk, LANES))
    extra = jnp.concatenate([packed, spots, jnp.zeros((16 - unit - 2 * nk, LANES), BF16)], axis=0)
    message = jnp.concatenate(
        [factors.transpose(1, 0, 2), jnp.broadcast_to(extra[None], (rows, 16, LANES))], axis=1)
    wide = jnp.repeat(energies.reshape(unit, nc), nvec, axis=1)
    vmem = pl.BlockSpec(memory_space=pltpu.VMEM)
    dma = pltpu.SemaphoreType.DMA
    points = cols * kb
    return pl.pallas_call(
        functools.partial(kernel, (rows, cols, nk, nv, nc, nvec, total, total // MX)),
        out_shape=(
            jax.ShapeDtypeStruct((nk, nb * nvec), F32),
            jax.ShapeDtypeStruct((nvec, nvec), F32),
        ),
        in_specs=[vmem] * 5,
        out_specs=(vmem, vmem),
        scratch_shapes=[
            pltpu.VMEM((cols, rows, 32, LANES), BF16),
            pltpu.VMEM((rows, nk, nb, LANES), BF16),
            pltpu.VMEM((batch, rows * 16), BF16),
            pltpu.VMEM((batch, rows * 16), BF16),
            pltpu.VMEM((LANES, nc * LANES), BF16),
            pltpu.VMEM((batch, kb * nvec), BF16),
            pltpu.VMEM((batch, batch), BF16),
            pltpu.VMEM((2 * points, count * 8), BF16),
            pltpu.VMEM((2 * LANES, LANES), BF16),
            pltpu.VMEM((cols, batch, LANES), BF16),
            pltpu.VMEM((cols, batch, LANES), F32),
            pltpu.VMEM((points, nvec, LANES), F32),
            pltpu.VMEM((cols, rows * 8, LANES), BF16),
            pltpu.VMEM((kb, points, LANES), F32),
            pltpu.VMEM((cols, nvec, LANES), F32),
            pltpu.VMEM((nc, rows, unit, nvec), F32),
            pltpu.VMEM((rows, unit, LANES), F32),
            pltpu.VMEM((rows, unit, LANES), F32),
            pltpu.VMEM((count, nvec // nc, LANES), F32),
            dma((cols, rows)), dma((cols, rows)),
            dma((rows,)), dma((rows,)),
            dma((cols,)), dma((cols,)),
            dma((count,)), dma((count,)),
            dma((rows,)), dma((rows,)),
        ],
        compiler_params=pltpu.CompilerParams(collective_id=0, has_side_effects=True),
    )(message, pair_exchange, wide, coulomb.reshape(1, planes), screening)


highest = lax.Precision.HIGHEST


def pair_factors(conduction, valence):
    count, valence_count, plane_count = valence.shape
    joined = (
        valence.astype(jnp.float32)[:, :, None, :] * conduction.astype(jnp.float32)[:, None, :, :]
    )
    return joined.reshape(count, valence_count * conduction.shape[1], plane_count).astype(
        jnp.bfloat16
    )


def transfer_index(rows_at, cols_at, mesh_cols):
    delta_first = jnp.mod(rows_at[:, None, 0] - cols_at[None, :, 0], MX)
    delta_second = jnp.mod(rows_at[:, None, 1] - cols_at[None, :, 1], mesh_cols)
    fold_first = jnp.minimum(delta_first, MX - delta_first)
    fold_second = jnp.minimum(delta_second, mesh_cols - delta_second)
    return (fold_first * (mesh_cols // 2 + 1) + fold_second).astype(jnp.int32)


def on_device(pair_exchange, conduction, valence, coulomb, screening, energies, vectors, k_coords):
    local_count, band_count, plane_count = pair_exchange.shape
    vector_count = vectors.shape[1] // band_count
    row_count = lax.axis_size("row")
    col_count = lax.axis_size("col")
    total_count = local_count * row_count * col_count
    mesh_cols = total_count // MX
    moving = vectors.reshape(local_count, band_count, vector_count)
    partial_density = jnp.einsum(
        "ktg,ktn->gn", pair_exchange, moving, preferred_element_type=jnp.float32
    )
    density = lax.psum(partial_density, ("row", "col"))
    block_size = 128
    sweeps = plane_count // block_size
    col_cond, col_val, col_vec, col_at = (
        lax.all_gather(conduction, "row", axis=0, tiled=True),
        lax.all_gather(valence, "row", axis=0, tiled=True),
        lax.all_gather(vectors, "row", axis=0, tiled=True),
        lax.all_gather(k_coords, "row", axis=0, tiled=True),
    )
    row_cond, row_val, row_at = (
        lax.all_gather(conduction, "col", axis=0, tiled=True),
        lax.all_gather(valence, "col", axis=0, tiled=True),
        lax.all_gather(k_coords, "col", axis=0, tiled=True),
    )
    row_pairs = pair_factors(row_cond, row_val)
    col_pairs = pair_factors(col_cond, col_val)
    indices = transfer_index(row_at, col_at, mesh_cols)
    col_moving = col_vec.reshape(-1, band_count, vector_count)

    def square_sweep(sweep_index, running):
        anchor = sweep_index * block_size
        coupling = jnp.take(
            lax.dynamic_slice_in_dim(screening, anchor, block_size, 1), indices, axis=0
        )
        row_block = lax.dynamic_slice_in_dim(row_pairs, anchor, block_size, 2)
        col_block = lax.dynamic_slice_in_dim(col_pairs, anchor, block_size, 2)
        col_proj = jnp.einsum(
            "ktg,ktn->kng", col_block, col_moving, preferred_element_type=jnp.float32
        )
        potential = jnp.einsum("ijg,jng->ing", coupling, col_proj, precision=highest)
        return running + jnp.einsum(
            "ktg,kng->ktn", row_block.astype(jnp.float32), potential, precision=highest
        )

    forward = lax.fori_loop(
        0,
        sweeps,
        square_sweep,
        jnp.zeros((row_pairs.shape[0], band_count, vector_count), jnp.float32),
    )
    owned = lax.psum_scatter(
        forward.reshape(col_count, local_count, band_count, vector_count),
        "col",
        scatter_dimension=0,
        tiled=True,
    )[0]
    moving_wide = moving.astype(jnp.float32)
    exchange_term = jnp.einsum(
        "ktg,gn->ktn", pair_exchange.astype(jnp.float32) * coulomb, density, precision=highest
    )
    applied = (
        energies[:, :, None] * moving_wide
        + 2.0 / (total_count * band_count) * exchange_term
        - owned / total_count
    )
    gram = jnp.einsum("ktm,ktn->mn", moving_wide, applied, precision=highest)
    alpha = lax.psum(gram, ("row", "col")) / (total_count * band_count)
    residual = applied - jnp.einsum("ktm,mn->ktn", moving_wide, alpha, precision=highest)
    return (residual.reshape(local_count, band_count * vector_count), alpha)


def fits(args, mesh):
    pair_exchange, conduction, valence, _, screening, _, vectors, _ = args
    rows, cols = mesh.shape["row"], mesh.shape["col"]
    points, nb, planes = pair_exchange.shape
    nk = points // (rows * cols)
    nv, nc = valence.shape[1], conduction.shape[1]
    nvec = vectors.shape[1] // nb
    return (
        planes == rows * LANES and nc * nvec == LANES and nk * nv == 8 and nk * (nv + nc) == 16
        and nk == 2 and nvec // nc == 8 and rows % 2 == 0 and screening.shape[0] <= LANES
        and points <= LANES
    )


def solution(mesh):
    in_specs = (
        P(("row", "col"), None, None),
        P(("row", "col"), None, None),
        P(("row", "col"), None, None),
        P(),
        P(),
        P(("row", "col"), None),
        P(("row", "col"), None),
        P(("row", "col"), None),
    )
    out_specs = (P(("row", "col"), None), P())

    def run(*args):
        body = fast_on_device if fits(args, mesh) else on_device
        return jax.shard_map(
            body, mesh=mesh, in_specs=in_specs, out_specs=out_specs, check_vma=False
        )(*args)

    return run
```

```python
import functools

import jax
import jax.numpy as jnp
from jax import lax
from jax.experimental import pallas as pl
from jax.experimental.pallas import tpu as pltpu
from jax.sharding import PartitionSpec as P

MX = 32
LANES = 128
MESH = pl.DeviceIdType.MESH
F32 = jnp.float32
BF16 = jnp.bfloat16


def split_pair(value):
    high = value.astype(BF16)
    return high, (value - high.astype(F32)).astype(BF16)


def dot(a, b, contract):
    return lax.dot_general(a, b, ((contract[0:1], contract[1:2]), ((), ())), preferred_element_type=F32)


def iota(shape, axis):
    return lax.broadcasted_iota(jnp.int32, shape, axis)


def one_hot(condition):
    return jnp.where(condition, 1.0, 0.0).astype(BF16)


def kernel(
    dims, px_hbm, cond_hbm, val_hbm, coulomb_hbm, screening_hbm, vec_hbm, energy_hbm, place_hbm,
    out_ref, alpha_ref,
    px_ref, cond_ref, val_ref, coulomb_ref, screening_ref, vec_ref, energy_ref, place_ref, msg_ref, wide_ref, load_sem,
    slots, px_slots, sel_v, sel_c, tile_m, block_m, perm, sel_k, screen, tiled, pairs, proj, coords, coupling,
    dens_slots, partial, out_send, out_slots, gram_slots,
    in_send, in_recv, px_send, px_recv, dens_send, dens_recv, gram_send, gram_recv, o_send, o_recv,
):
    rows, cols, nk, nv, nc, nvec, total, mesh_cols = dims
    row, col = lax.axis_index("row"), lax.axis_index("col")
    me = row * cols + col
    count = rows * cols
    kb = rows * nk
    nb = nv * nc
    unit = nk * nv
    per = kb * nv
    batch = per * nc

    def other(step):
        peer = lax.rem(me + step, count)
        return peer // cols, lax.rem(peer, cols)

    barrier = pltpu.get_barrier_semaphore()

    def greet(step, carry):
        pr, pc = other(step)
        pl.semaphore_signal(barrier, inc=1, device_id=(pr, pc), device_id_type=MESH)
        return carry

    lax.fori_loop(1, count, greet, 0)

    mine = pl.ds(pl.multiple_of(row * LANES, LANES), LANES)
    loads = [
        pltpu.make_async_copy(src, dst, load_sem.at[at])
        for at, (src, dst) in enumerate((
            (val_hbm, val_ref), (cond_hbm, cond_ref), (vec_hbm, vec_ref), (place_hbm, place_ref), (energy_hbm, energy_ref), (px_hbm, px_ref),
            (screening_hbm.at[:, mine], screening_ref), (coulomb_hbm.at[:, mine], coulomb_ref)))
    ]
    for load in loads:
        load.start()
    for load in loads[:5]:
        load.wait()
    row8 = iota((8, LANES), 0)
    lane8 = iota((8, LANES), 1)
    spots = jnp.zeros((8, LANES), F32)
    for axis in range(2):
        for k in range(nk):
            spots = jnp.where(row8 == axis * nk + k, place_ref[k, axis].astype(F32), spots)
    energy = jnp.zeros((8, LANES), F32)
    for k in range(nk):
        for t in range(nb):
            energy = jnp.where((row8 == k * nv + t // nc) & (lane8 // nvec == t % nc), energy_ref[k, t], energy)
    vec = vec_ref[...].astype(F32)
    packed_own = jnp.concatenate(
        [vec[k:k + 1, j * LANES:(j + 1) * LANES] for k in range(nk) for j in range(nv)], axis=0)
    wide_ref[0] = packed_own
    wide_ref[1] = energy * packed_own
    message = jnp.concatenate(
        [ref[k].astype(F32) for k in range(nk) for ref in (val_ref, cond_ref)], axis=0).astype(BF16)
    extra = jnp.concatenate([packed_own, spots], axis=0).astype(BF16)
    for r in range(rows):
        msg_ref[r, 0:16] = message[:, r * LANES:(r + 1) * LANES]
        msg_ref[r, 16:32] = extra

    at = iota((batch, rows * 16), 0)
    to = iota((batch, rows * 16), 1)
    base = (at // unit) % rows * 16 + (at // nv) % nk * 8
    sel_v[...] = one_hot(to == base + at % nv)
    sel_c[...] = one_hot(to == base + nv + at // per)
    at = iota((LANES, nc * LANES), 0)
    to = iota((LANES, nc * LANES), 1)
    tile_m[...] = one_hot((at // nvec == to // LANES) & (at % nvec == to % nvec))
    at = iota((batch, kb * nvec), 0)
    to = iota((batch, kb * nvec), 1)
    block_m[...] = one_hot((at // nv) % kb == to // nvec)
    at = iota((batch, rows * nk * nb), 0)
    to = iota((batch, rows * nk * nb), 1)
    perm[...] = one_hot(to == (at // nv) % kb * nb + at % nv * nc + at // per)
    at = iota((2 * cols * kb, count * 8), 0)
    to = iota((2 * cols * kb, count * 8), 1)
    point = at % (cols * kb)
    sel_k[...] = one_hot(to == point // nk * 8 + at // (cols * kb) * nk + point % nk)
    for load in loads[5:]:
        load.wait()
    high, low = split_pair(jnp.concatenate(
        [screening_ref[...], jnp.zeros((LANES - screening_ref.shape[0], LANES), F32)], axis=0))
    screen[0:LANES] = high
    screen[LANES:2 * LANES] = low

    pl.semaphore_wait(barrier, count - 1)

    def in_copy(step):
        pr, pc = other(step)
        return pltpu.make_async_remote_copy(
            src_ref=msg_ref.at[pr], dst_ref=slots.at[col, row],
            send_sem=in_send.at[pc, pr], recv_sem=in_recv.at[col, row],
            device_id=(pr, pc), device_id_type=MESH)

    def px_copy(step):
        pr = lax.rem(row + step, rows)
        return pltpu.make_async_remote_copy(
            src_ref=px_ref.at[:, :, pl.ds(pl.multiple_of(pr * LANES, LANES), LANES)], dst_ref=px_slots.at[row],
            send_sem=px_send.at[pr], recv_sem=px_recv.at[row],
            device_id=(pr, col), device_id_type=MESH)

    def dens_copy(step):
        pc = lax.rem(col + step, cols)
        return pltpu.make_async_remote_copy(
            src_ref=dens_slots.at[col], dst_ref=dens_slots.at[col],
            send_sem=dens_send.at[pc], recv_sem=dens_recv.at[col],
            device_id=(row, pc), device_id_type=MESH)

    def gram_copy(step):
        pr, pc = other(step)
        return pltpu.make_async_remote_copy(
            src_ref=gram_slots.at[me], dst_ref=gram_slots.at[me],
            send_sem=gram_send.at[pr * cols + pc], recv_sem=gram_recv.at[me],
            device_id=(pr, pc), device_id_type=MESH)

    def o_copy(step):
        pr = lax.rem(row + step, rows)
        return pltpu.make_async_remote_copy(
            src_ref=out_send.at[pr], dst_ref=out_slots.at[row],
            send_sem=o_send.at[pr], recv_sem=o_recv.at[row],
            device_id=(pr, col), device_id_type=MESH)

    def start_all(copy, end):
        def body(step, carry):
            copy(step).start()
            return carry
        lax.fori_loop(1, end, body, 0)

    def landed(ref, sem):
        pltpu.make_async_copy(ref, ref, sem).wait()

    start_all(px_copy, rows)
    start_all(in_copy, count)
    slots[col, row] = msg_ref[row]
    px_slots[row] = px_ref[:, :, mine]

    def take_batch(which):
        def wait_one(r, carry):
            @pl.when((r != row) | (which != col))
            def _():
                landed(slots.at[which, r], in_recv.at[which, r])
            return carry
        lax.fori_loop(0, rows, wait_one, 0)
        got = slots[which]
        factors = got[:, 0:16, :].reshape(rows * 16, LANES)
        rest = got[:, 16:32, :].astype(F32)
        packed = rest[:, 0:8, :].reshape(per, LANES).astype(BF16)
        coords[which] = rest[:, 8:16, :].reshape(rows * 8, LANES).astype(BF16)
        wide = dot(packed, tile_m[...], (1, 0)).astype(BF16)
        stacked = jnp.concatenate([wide[:, s * LANES:(s + 1) * LANES] for s in range(nc)], axis=0)
        tiled[which] = stacked
        joined = (dot(sel_v[...], factors, (1, 0)) * dot(sel_c[...], factors, (1, 0))).astype(BF16)
        pairs[which] = joined.astype(F32)
        spread = jnp.concatenate([stacked] * (kb * nvec // LANES), axis=1) * block_m[...]
        projected = dot(spread, joined, (0, 0))
        proj[pl.ds(which * kb, kb)] = projected.reshape(kb, nvec, LANES)

    take_batch(col)

    def px_wait(step, carry):
        r = lax.rem(row + step, rows)
        landed(px_slots.at[r], px_recv.at[r])
        return carry

    lax.fori_loop(1, rows, px_wait, 0)
    px = dot(perm[...], px_slots[...].reshape(rows * nk * nb, LANES), (1, 0)).astype(BF16)
    own_x = tiled[col][:, 0:nvec]
    dens_slots[col] = dot(own_x, px, (0, 0))
    start_all(dens_copy, cols)

    def rest_batches(step, carry):
        take_batch(lax.rem(col + step, cols))
        return carry

    lax.fori_loop(1, cols, rest_batches, 0)

    place = dot(sel_k[...], coords[...].reshape(count * 8, LANES), (1, 0))
    points = cols * kb
    first, second = place[0:points], place[points:2 * points]
    lane = iota((points, LANES), 1).astype(F32)
    coupling[0, 0:points] = first
    coupling[1, 0:points] = second
    start = pl.multiple_of(col * kb, kb)
    own_first = coupling[0, pl.ds(start, kb), :]
    own_second = coupling[1, pl.ds(start, kb), :]
    hots = []
    for i in range(kb):
        da = jnp.abs(own_first[i:i + 1] - first)
        db = jnp.abs(own_second[i:i + 1] - second)
        q = jnp.minimum(da, MX - da) * (mesh_cols // 2 + 1) + jnp.minimum(db, mesh_cols - db)
        hots.append(one_hot(q == lane))
    for i in range(kb):
        coupling[i] = dot(jnp.concatenate([hots[i], hots[i]], axis=1), screen[...], (1, 0))

    def dens_wait(step, carry):
        c = lax.rem(col + step, cols)
        landed(dens_slots.at[c], dens_recv.at[c])
        return carry

    lax.fori_loop(1, cols, dens_wait, 0)
    density = dens_slots[0]
    for c in range(1, cols):
        density = density + dens_slots[c]
    high, low = split_pair(density * coulomb_ref[...] * (2.0 / (total * nb)))
    partial[...] = (dot(px, high, (1, 1)) + dot(px, low, (1, 1))).reshape(nc, rows, unit, nvec)

    wide_own = wide_ref[1]
    for s in range(nc):
        partial[s, row] = partial[s, row] + wide_own[:, s * nvec:(s + 1) * nvec]

    group = 4
    row_k = (iota((nc * unit, LANES), 0) // nv) % nk
    potentials = []
    for block in range(kb // group):
        def gather(j, sums):
            term = proj[j]
            return tuple(
                sums[u] + coupling[block * group + u, pl.ds(j, 1), :] * term for u in range(group))
        potentials += list(lax.fori_loop(
            0, points, gather, tuple(jnp.zeros((nvec, LANES), F32) for _ in range(group)), unroll=8))
    for r in range(rows):
        mine_pairs = pairs[col].reshape(nc, rows, unit, LANES)[:, r].reshape(nc * unit, LANES)
        left = jnp.concatenate(
            [jnp.where(row_k == k, mine_pairs, 0.0) for k in range(nk)], axis=1).astype(BF16)
        high, low = split_pair(jnp.concatenate([potentials[r * nk + k] for k in range(nk)], axis=1))
        direct = dot(left, high, (1, 1)) + dot(left, low, (1, 1))
        for s in range(nc):
            partial[s, r] = partial[s, r] - direct[s * unit:(s + 1) * unit] * (1.0 / total)

    whole = partial[...]
    packed = jnp.concatenate([whole[s].reshape(per, nvec) for s in range(nc)], axis=1)
    out_send[...] = packed.reshape(rows, unit, LANES)
    start_all(o_copy, rows)
    high, low = split_pair(whole.reshape(batch, nvec))
    gram = dot(own_x, high, (0, 0)) + dot(own_x, low, (0, 0))
    step = nvec // nc
    gram_slots[me] = jnp.concatenate([gram[s * step:(s + 1) * step] for s in range(nc)], axis=1)
    start_all(gram_copy, count)

    def o_wait(d, acc):
        r = lax.rem(row + d, rows)
        landed(out_slots.at[r], o_recv.at[r])
        return acc + out_slots[r]

    applied = lax.fori_loop(1, rows, o_wait, out_send[row])

    def gram_wait(d, carry):
        p = lax.rem(me + d, count)
        landed(gram_slots.at[p], gram_recv.at[p])
        return carry

    lax.fori_loop(1, count, gram_wait, 0)
    sums = jnp.sum(gram_slots[...], axis=0) * (1.0 / (total * nb))
    alpha = jnp.concatenate([sums[:, s * nvec:(s + 1) * nvec] for s in range(nc)], axis=0)
    alpha_ref[...] = alpha
    own = wide_ref[0]
    own_rows = jnp.concatenate([own[:, s * nvec:(s + 1) * nvec] for s in range(nc)], axis=0).astype(BF16)
    high, low = split_pair(alpha)
    taken = dot(own_rows, high, (1, 0)) + dot(own_rows, low, (1, 0))
    residual = applied - jnp.concatenate([taken[s * unit:(s + 1) * unit] for s in range(nc)], axis=1)
    for j in range(nv):
        out_ref[:, j * LANES:(j + 1) * LANES] = jnp.concatenate(
            [residual[k * nv + j:k * nv + j + 1] for k in range(nk)], axis=0)

    def drain(copy, end):
        def body(d, carry):
            copy(d).wait_send()
            return carry
        lax.fori_loop(1, end, body, 0)

    drain(in_copy, count)
    drain(px_copy, rows)
    drain(dens_copy, cols)
    drain(o_copy, rows)
    drain(gram_copy, count)


def fast_on_device(pair_exchange, conduction, valence, coulomb, screening, energies, vectors, k_coords):
    nk, nb, planes = pair_exchange.shape
    nv, nc = valence.shape[1], conduction.shape[1]
    nvec = vectors.shape[1] // nb
    rows, cols = lax.axis_size("row"), lax.axis_size("col")
    count = rows * cols
    total = nk * count
    unit = nk * nv
    kb = rows * nk
    batch = kb * nb
    vmem = pl.BlockSpec(memory_space=pltpu.VMEM)
    dma = pltpu.SemaphoreType.DMA
    points = cols * kb
    return pl.pallas_call(
        functools.partial(kernel, (rows, cols, nk, nv, nc, nvec, total, total // MX)),
        out_shape=(
            pltpu.VMEM((nk, nb * nvec), F32),
            pltpu.VMEM((nvec, nvec), F32),
        ),
        in_specs=[pl.BlockSpec(memory_space=pl.ANY)] * 8,
        out_specs=(vmem, vmem),
        scratch_shapes=[
            pltpu.VMEM(pair_exchange.shape, BF16),
            pltpu.VMEM(conduction.shape, BF16),
            pltpu.VMEM(valence.shape, BF16),
            pltpu.VMEM((1, LANES), F32),
            pltpu.VMEM((screening.shape[0], LANES), F32),
            pltpu.VMEM(vectors.shape, BF16),
            pltpu.SMEM(energies.shape, F32),
            pltpu.SMEM(k_coords.shape, jnp.int32),
            pltpu.VMEM((rows, 32, LANES), BF16),
            pltpu.VMEM((2, unit, LANES), F32),
            dma((8,)),
            pltpu.VMEM((cols, rows, 32, LANES), BF16),
            pltpu.VMEM((rows, nk, nb, LANES), BF16),
            pltpu.VMEM((batch, rows * 16), BF16),
            pltpu.VMEM((batch, rows * 16), BF16),
            pltpu.VMEM((LANES, nc * LANES), BF16),
            pltpu.VMEM((batch, kb * nvec), BF16),
            pltpu.VMEM((batch, batch), BF16),
            pltpu.VMEM((2 * points, count * 8), BF16),
            pltpu.VMEM((2 * LANES, LANES), BF16),
            pltpu.VMEM((cols, batch, LANES), BF16),
            pltpu.VMEM((cols, batch, LANES), F32),
            pltpu.VMEM((points, nvec, LANES), F32),
            pltpu.VMEM((cols, rows * 8, LANES), BF16),
            pltpu.VMEM((kb, points, LANES), F32),
            pltpu.VMEM((cols, nvec, LANES), F32),
            pltpu.VMEM((nc, rows, unit, nvec), F32),
            pltpu.VMEM((rows, unit, LANES), F32),
            pltpu.VMEM((rows, unit, LANES), F32),
            pltpu.VMEM((count, nvec // nc, LANES), F32),
            dma((cols, rows)), dma((cols, rows)),
            dma((rows,)), dma((rows,)),
            dma((cols,)), dma((cols,)),
            dma((count,)), dma((count,)),
            dma((rows,)), dma((rows,)),
        ],
        compiler_params=pltpu.CompilerParams(collective_id=0, has_side_effects=True),
    )(pair_exchange, conduction, valence, coulomb.reshape(1, planes), screening, vectors, energies, k_coords)


highest = lax.Precision.HIGHEST


def pair_factors(conduction, valence):
    count, valence_count, plane_count = valence.shape
    joined = (
        valence.astype(jnp.float32)[:, :, None, :] * conduction.astype(jnp.float32)[:, None, :, :]
    )
    return joined.reshape(count, valence_count * conduction.shape[1], plane_count).astype(
        jnp.bfloat16
    )


def transfer_index(rows_at, cols_at, mesh_cols):
    delta_first = jnp.mod(rows_at[:, None, 0] - cols_at[None, :, 0], MX)
    delta_second = jnp.mod(rows_at[:, None, 1] - cols_at[None, :, 1], mesh_cols)
    fold_first = jnp.minimum(delta_first, MX - delta_first)
    fold_second = jnp.minimum(delta_second, mesh_cols - delta_second)
    return (fold_first * (mesh_cols // 2 + 1) + fold_second).astype(jnp.int32)


def on_device(pair_exchange, conduction, valence, coulomb, screening, energies, vectors, k_coords):
    local_count, band_count, plane_count = pair_exchange.shape
    vector_count = vectors.shape[1] // band_count
    row_count = lax.axis_size("row")
    col_count = lax.axis_size("col")
    total_count = local_count * row_count * col_count
    mesh_cols = total_count // MX
    moving = vectors.reshape(local_count, band_count, vector_count)
    partial_density = jnp.einsum(
        "ktg,ktn->gn", pair_exchange, moving, preferred_element_type=jnp.float32
    )
    density = lax.psum(partial_density, ("row", "col"))
    block_size = 128
    sweeps = plane_count // block_size
    col_cond, col_val, col_vec, col_at = (
        lax.all_gather(conduction, "row", axis=0, tiled=True),
        lax.all_gather(valence, "row", axis=0, tiled=True),
        lax.all_gather(vectors, "row", axis=0, tiled=True),
        lax.all_gather(k_coords, "row", axis=0, tiled=True),
    )
    row_cond, row_val, row_at = (
        lax.all_gather(conduction, "col", axis=0, tiled=True),
        lax.all_gather(valence, "col", axis=0, tiled=True),
        lax.all_gather(k_coords, "col", axis=0, tiled=True),
    )
    row_pairs = pair_factors(row_cond, row_val)
    col_pairs = pair_factors(col_cond, col_val)
    indices = transfer_index(row_at, col_at, mesh_cols)
    col_moving = col_vec.reshape(-1, band_count, vector_count)

    def square_sweep(sweep_index, running):
        anchor = sweep_index * block_size
        coupling = jnp.take(
            lax.dynamic_slice_in_dim(screening, anchor, block_size, 1), indices, axis=0
        )
        row_block = lax.dynamic_slice_in_dim(row_pairs, anchor, block_size, 2)
        col_block = lax.dynamic_slice_in_dim(col_pairs, anchor, block_size, 2)
        col_proj = jnp.einsum(
            "ktg,ktn->kng", col_block, col_moving, preferred_element_type=jnp.float32
        )
        potential = jnp.einsum("ijg,jng->ing", coupling, col_proj, precision=highest)
        return running + jnp.einsum(
            "ktg,kng->ktn", row_block.astype(jnp.float32), potential, precision=highest
        )

    forward = lax.fori_loop(
        0,
        sweeps,
        square_sweep,
        jnp.zeros((row_pairs.shape[0], band_count, vector_count), jnp.float32),
    )
    owned = lax.psum_scatter(
        forward.reshape(col_count, local_count, band_count, vector_count),
        "col",
        scatter_dimension=0,
        tiled=True,
    )[0]
    moving_wide = moving.astype(jnp.float32)
    exchange_term = jnp.einsum(
        "ktg,gn->ktn", pair_exchange.astype(jnp.float32) * coulomb, density, precision=highest
    )
    applied = (
        energies[:, :, None] * moving_wide
        + 2.0 / (total_count * band_count) * exchange_term
        - owned / total_count
    )
    gram = jnp.einsum("ktm,ktn->mn", moving_wide, applied, precision=highest)
    alpha = lax.psum(gram, ("row", "col")) / (total_count * band_count)
    residual = applied - jnp.einsum("ktm,mn->ktn", moving_wide, alpha, precision=highest)
    return (residual.reshape(local_count, band_count * vector_count), alpha)


def fits(args, mesh):
    pair_exchange, conduction, valence, _, screening, _, vectors, _ = args
    rows, cols = mesh.shape["row"], mesh.shape["col"]
    points, nb, planes = pair_exchange.shape
    nk = points // (rows * cols)
    nv, nc = valence.shape[1], conduction.shape[1]
    nvec = vectors.shape[1] // nb
    return (
        planes == rows * LANES and nc * nvec == LANES and nk * nv == 8 and nk * (nv + nc) == 16
        and nk == 2 and nvec // nc == 8 and rows % 2 == 0 and screening.shape[0] <= LANES
        and points <= LANES
    )


def solution(mesh):
    in_specs = (
        P(("row", "col"), None, None),
        P(("row", "col"), None, None),
        P(("row", "col"), None, None),
        P(),
        P(),
        P(("row", "col"), None),
        P(("row", "col"), None),
        P(("row", "col"), None),
    )
    out_specs = (P(("row", "col"), None), P())

    def run(*args):
        body = fast_on_device if fits(args, mesh) else on_device
        return jax.shard_map(
            body, mesh=mesh, in_specs=in_specs, out_specs=out_specs, check_vma=False
        )(*args)

    return run
```

```python
import functools

import jax
import jax.numpy as jnp
from jax import lax
from jax.experimental import pallas as pl
from jax.experimental.pallas import tpu as pltpu
from jax.sharding import PartitionSpec as P

MX = 32
LANES = 128
MESH = pl.DeviceIdType.MESH
F32 = jnp.float32
BF16 = jnp.bfloat16


def split_pair(value):
    high = value.astype(BF16)
    return high, (value - high.astype(F32)).astype(BF16)


def dot(a, b, contract):
    return lax.dot_general(a, b, ((contract[0:1], contract[1:2]), ((), ())), preferred_element_type=F32)


def iota(shape, axis):
    return lax.broadcasted_iota(jnp.int32, shape, axis)


def one_hot(condition):
    return jnp.where(condition, 1.0, 0.0).astype(BF16)


def kernel(
    dims, px_hbm, cond_hbm, val_hbm, coulomb_hbm, screening_hbm, vec_hbm, energy_hbm, place_hbm,
    out_ref, alpha_ref,
    px_ref, cond_ref, val_ref, coulomb_ref, screening_ref, vec_ref, energy_ref, place_ref, msg_ref, wide_ref, load_sem,
    slots, px_slots, sel_v, sel_c, tile_m, block_m, perm, sel_k, screen, tiled, pairs, proj, coords, coupling,
    dens_slots, partial, out_send, out_slots, gram_slots,
    in_send, in_recv, px_send, px_recv, dens_send, dens_recv, gram_send, gram_recv, o_send, o_recv,
):
    rows, cols, nk, nv, nc, nvec, total, mesh_cols = dims
    row, col = lax.axis_index("row"), lax.axis_index("col")
    me = row * cols + col
    count = rows * cols
    kb = rows * nk
    nb = nv * nc
    unit = nk * nv
    per = kb * nv
    batch = per * nc

    def other(step):
        peer = lax.rem(me + step, count)
        return peer // cols, lax.rem(peer, cols)

    barrier = pltpu.get_barrier_semaphore()

    for step in range(1, rows):
        pl.semaphore_signal(barrier, inc=1, device_id=(lax.rem(row + step, rows), col), device_id_type=MESH)
    for step in range(1, cols):
        pl.semaphore_signal(barrier, inc=1, device_id=(row, lax.rem(col + step, cols)), device_id_type=MESH)

    mine = pl.ds(pl.multiple_of(row * LANES, LANES), LANES)
    loads = [
        pltpu.make_async_copy(src, dst, load_sem.at[at])
        for at, (src, dst) in enumerate((
            (val_hbm, val_ref), (cond_hbm, cond_ref), (vec_hbm, vec_ref), (place_hbm, place_ref), (energy_hbm, energy_ref), (px_hbm, px_ref),
            (screening_hbm.at[:, mine], screening_ref), (coulomb_hbm.at[:, mine], coulomb_ref)))
    ]
    for load in loads:
        load.start()
    for load in loads[:5]:
        load.wait()
    row8 = iota((8, LANES), 0)
    lane8 = iota((8, LANES), 1)
    spots = jnp.zeros((8, LANES), F32)
    for axis in range(2):
        for k in range(nk):
            spots = jnp.where(row8 == axis * nk + k, place_ref[k, axis].astype(F32), spots)
    energy = jnp.zeros((8, LANES), F32)
    for k in range(nk):
        for t in range(nb):
            energy = jnp.where((row8 == k * nv + t // nc) & (lane8 // nvec == t % nc), energy_ref[k, t], energy)
    vec = vec_ref[...].astype(F32)
    packed_own = jnp.concatenate(
        [vec[k:k + 1, j * LANES:(j + 1) * LANES] for k in range(nk) for j in range(nv)], axis=0)
    wide_ref[0] = packed_own
    wide_ref[1] = energy * packed_own
    message = jnp.concatenate(
        [ref[k].astype(F32) for k in range(nk) for ref in (val_ref, cond_ref)], axis=0).astype(BF16)
    extra = jnp.concatenate([packed_own, spots], axis=0).astype(BF16)
    for r in range(rows):
        msg_ref[r, 0:16] = message[:, r * LANES:(r + 1) * LANES]
        msg_ref[r, 16:32] = extra

    at = iota((batch, rows * 16), 0)
    to = iota((batch, rows * 16), 1)
    base = (at // unit) % rows * 16 + (at // nv) % nk * 8
    sel_v[...] = one_hot(to == base + at % nv)
    sel_c[...] = one_hot(to == base + nv + at // per)
    at = iota((LANES, nc * LANES), 0)
    to = iota((LANES, nc * LANES), 1)
    tile_m[...] = one_hot((at // nvec == to // LANES) & (at % nvec == to % nvec))
    at = iota((batch, kb * nvec), 0)
    to = iota((batch, kb * nvec), 1)
    block_m[...] = one_hot((at // nv) % kb == to // nvec)
    at = iota((batch, rows * nk * nb), 0)
    to = iota((batch, rows * nk * nb), 1)
    perm[...] = one_hot(to == (at // nv) % kb * nb + at % nv * nc + at // per)
    at = iota((2 * cols * kb, count * 8), 0)
    to = iota((2 * cols * kb, count * 8), 1)
    point = at % (cols * kb)
    sel_k[...] = one_hot(to == point // nk * 8 + at // (cols * kb) * nk + point % nk)
    for load in loads[5:]:
        load.wait()
    slots[col, row] = msg_ref[row]
    high, low = split_pair(jnp.concatenate(
        [screening_ref[...], jnp.zeros((LANES - screening_ref.shape[0], LANES), F32)], axis=0))
    screen[0:LANES] = high
    screen[LANES:2 * LANES] = low

    pl.semaphore_wait(barrier, rows + cols - 2)

    def in_copy(step):
        pr = lax.rem(row + step, rows)
        return pltpu.make_async_remote_copy(
            src_ref=msg_ref.at[pr], dst_ref=slots.at[col, row],
            send_sem=in_send.at[col, pr], recv_sem=in_recv.at[col, row],
            device_id=(pr, col), device_id_type=MESH)

    def relay_copy(r, step):
        pc = lax.rem(col + step, cols)
        return pltpu.make_async_remote_copy(
            src_ref=slots.at[col, r], dst_ref=slots.at[col, r],
            send_sem=in_send.at[pc, r], recv_sem=in_recv.at[col, r],
            device_id=(row, pc), device_id_type=MESH)

    def px_copy(step):
        pr = lax.rem(row + step, rows)
        return pltpu.make_async_remote_copy(
            src_ref=px_ref.at[:, :, pl.ds(pl.multiple_of(pr * LANES, LANES), LANES)], dst_ref=px_slots.at[row],
            send_sem=px_send.at[pr], recv_sem=px_recv.at[row],
            device_id=(pr, col), device_id_type=MESH)

    def dens_copy(step):
        pc = lax.rem(col + step, cols)
        return pltpu.make_async_remote_copy(
            src_ref=dens_slots.at[col], dst_ref=dens_slots.at[col],
            send_sem=dens_send.at[pc], recv_sem=dens_recv.at[col],
            device_id=(row, pc), device_id_type=MESH)

    def gram_copy(step):
        pr, pc = other(step)
        return pltpu.make_async_remote_copy(
            src_ref=gram_slots.at[me], dst_ref=gram_slots.at[me],
            send_sem=gram_send.at[pr * cols + pc], recv_sem=gram_recv.at[me],
            device_id=(pr, pc), device_id_type=MESH)

    def o_copy(step):
        pr = lax.rem(row + step, rows)
        return pltpu.make_async_remote_copy(
            src_ref=out_send.at[pr], dst_ref=out_slots.at[row],
            send_sem=o_send.at[pr], recv_sem=o_recv.at[row],
            device_id=(pr, col), device_id_type=MESH)

    def start_all(copy, end):
        def body(step, carry):
            copy(step).start()
            return carry
        lax.fori_loop(1, end, body, 0)

    def landed(ref, sem):
        pltpu.make_async_copy(ref, ref, sem).wait()

    start_all(in_copy, rows)
    start_all(px_copy, rows)
    px_slots[row] = px_ref[:, :, mine]

    def relay(d, carry):
        r = lax.rem(row + d, rows)
        landed(slots.at[col, r], in_recv.at[col, r])
        for step in range(1, cols):
            relay_copy(r, step).start()
        return carry

    for step in range(1, cols):
        relay_copy(row, step).start()
    lax.fori_loop(1, rows, relay, 0)

    def take_batch(which):
        got = slots[which]
        factors = got[:, 0:16, :].reshape(rows * 16, LANES)
        rest = got[:, 16:32, :].astype(F32)
        packed = rest[:, 0:8, :].reshape(per, LANES).astype(BF16)
        coords[which] = rest[:, 8:16, :].reshape(rows * 8, LANES).astype(BF16)
        wide = dot(packed, tile_m[...], (1, 0)).astype(BF16)
        stacked = jnp.concatenate([wide[:, s * LANES:(s + 1) * LANES] for s in range(nc)], axis=0)
        tiled[which] = stacked
        joined = (dot(sel_v[...], factors, (1, 0)) * dot(sel_c[...], factors, (1, 0))).astype(BF16)
        pairs[which] = joined.astype(F32)
        spread = jnp.concatenate([stacked] * (kb * nvec // LANES), axis=1) * block_m[...]
        projected = dot(spread, joined, (0, 0))
        proj[pl.ds(which * kb, kb)] = projected.reshape(kb, nvec, LANES)

    take_batch(col)

    def px_wait(step, carry):
        r = lax.rem(row + step, rows)
        landed(px_slots.at[r], px_recv.at[r])
        return carry

    lax.fori_loop(1, rows, px_wait, 0)
    px = dot(perm[...], px_slots[...].reshape(rows * nk * nb, LANES), (1, 0)).astype(BF16)
    own_x = tiled[col][:, 0:nvec]
    dens_slots[col] = dot(own_x, px, (0, 0))
    start_all(dens_copy, cols)

    def rest_batches(step, carry):
        c = lax.rem(col + step, cols)

        def wait_one(r, inner):
            landed(slots.at[c, r], in_recv.at[c, r])
            return inner

        lax.fori_loop(0, rows, wait_one, 0)
        take_batch(c)
        return carry

    lax.fori_loop(1, cols, rest_batches, 0)

    place = dot(sel_k[...], coords[...].reshape(count * 8, LANES), (1, 0))
    points = cols * kb
    first, second = place[0:points], place[points:2 * points]
    lane = iota((points, LANES), 1).astype(F32)
    coupling[0, 0:points] = first
    coupling[1, 0:points] = second
    start = pl.multiple_of(col * kb, kb)
    own_first = coupling[0, pl.ds(start, kb), :]
    own_second = coupling[1, pl.ds(start, kb), :]
    hots = []
    for i in range(kb):
        da = jnp.abs(own_first[i:i + 1] - first)
        db = jnp.abs(own_second[i:i + 1] - second)
        q = jnp.minimum(da, MX - da) * (mesh_cols // 2 + 1) + jnp.minimum(db, mesh_cols - db)
        hots.append(one_hot(q == lane))
    for i in range(kb):
        coupling[i] = dot(jnp.concatenate([hots[i], hots[i]], axis=1), screen[...], (1, 0))

    def dens_wait(step, carry):
        c = lax.rem(col + step, cols)
        landed(dens_slots.at[c], dens_recv.at[c])
        return carry

    lax.fori_loop(1, cols, dens_wait, 0)
    density = dens_slots[0]
    for c in range(1, cols):
        density = density + dens_slots[c]
    high, low = split_pair(density * coulomb_ref[...] * (2.0 / (total * nb)))
    partial[...] = (dot(px, high, (1, 1)) + dot(px, low, (1, 1))).reshape(nc, rows, unit, nvec)

    wide_own = wide_ref[1]
    for s in range(nc):
        partial[s, row] = partial[s, row] + wide_own[:, s * nvec:(s + 1) * nvec]

    group = 4
    row_k = (iota((nc * unit, LANES), 0) // nv) % nk
    potentials = []
    for block in range(kb // group):
        def gather(j, sums):
            term = proj[j]
            return tuple(
                sums[u] + coupling[block * group + u, pl.ds(j, 1), :] * term for u in range(group))
        potentials += list(lax.fori_loop(
            0, points, gather, tuple(jnp.zeros((nvec, LANES), F32) for _ in range(group)), unroll=8))
    for r in range(rows):
        mine_pairs = pairs[col].reshape(nc, rows, unit, LANES)[:, r].reshape(nc * unit, LANES)
        left = jnp.concatenate(
            [jnp.where(row_k == k, mine_pairs, 0.0) for k in range(nk)], axis=1).astype(BF16)
        high, low = split_pair(jnp.concatenate([potentials[r * nk + k] for k in range(nk)], axis=1))
        direct = dot(left, high, (1, 1)) + dot(left, low, (1, 1))
        for s in range(nc):
            partial[s, r] = partial[s, r] - direct[s * unit:(s + 1) * unit] * (1.0 / total)

    whole = partial[...]
    packed = jnp.concatenate([whole[s].reshape(per, nvec) for s in range(nc)], axis=1)
    out_send[...] = packed.reshape(rows, unit, LANES)
    start_all(o_copy, rows)
    high, low = split_pair(whole.reshape(batch, nvec))
    gram = dot(own_x, high, (0, 0)) + dot(own_x, low, (0, 0))
    step = nvec // nc
    gram_slots[me] = jnp.concatenate([gram[s * step:(s + 1) * step] for s in range(nc)], axis=1)
    start_all(gram_copy, count)

    def o_wait(d, acc):
        r = lax.rem(row + d, rows)
        landed(out_slots.at[r], o_recv.at[r])
        return acc + out_slots[r]

    applied = lax.fori_loop(1, rows, o_wait, out_send[row])

    def gram_wait(d, carry):
        p = lax.rem(me + d, count)
        landed(gram_slots.at[p], gram_recv.at[p])
        return carry

    lax.fori_loop(1, count, gram_wait, 0)
    sums = jnp.sum(gram_slots[...], axis=0) * (1.0 / (total * nb))
    alpha = jnp.concatenate([sums[:, s * nvec:(s + 1) * nvec] for s in range(nc)], axis=0)
    alpha_ref[...] = alpha
    own = wide_ref[0]
    own_rows = jnp.concatenate([own[:, s * nvec:(s + 1) * nvec] for s in range(nc)], axis=0).astype(BF16)
    high, low = split_pair(alpha)
    taken = dot(own_rows, high, (1, 0)) + dot(own_rows, low, (1, 0))
    residual = applied - jnp.concatenate([taken[s * unit:(s + 1) * unit] for s in range(nc)], axis=1)
    for j in range(nv):
        out_ref[:, j * LANES:(j + 1) * LANES] = jnp.concatenate(
            [residual[k * nv + j:k * nv + j + 1] for k in range(nk)], axis=0)

    def drain(copy, end):
        def body(d, carry):
            copy(d).wait_send()
            return carry
        lax.fori_loop(1, end, body, 0)

    drain(in_copy, rows)

    def drain_relay(r, carry):
        for step in range(1, cols):
            relay_copy(r, step).wait_send()
        return carry

    lax.fori_loop(0, rows, drain_relay, 0)
    drain(px_copy, rows)
    drain(dens_copy, cols)
    drain(o_copy, rows)
    drain(gram_copy, count)


def fast_on_device(pair_exchange, conduction, valence, coulomb, screening, energies, vectors, k_coords):
    nk, nb, planes = pair_exchange.shape
    nv, nc = valence.shape[1], conduction.shape[1]
    nvec = vectors.shape[1] // nb
    rows, cols = lax.axis_size("row"), lax.axis_size("col")
    count = rows * cols
    total = nk * count
    unit = nk * nv
    kb = rows * nk
    batch = kb * nb
    vmem = pl.BlockSpec(memory_space=pltpu.VMEM)
    dma = pltpu.SemaphoreType.DMA
    points = cols * kb
    return pl.pallas_call(
        functools.partial(kernel, (rows, cols, nk, nv, nc, nvec, total, total // MX)),
        out_shape=(
            pltpu.VMEM((nk, nb * nvec), F32),
            pltpu.VMEM((nvec, nvec), F32),
        ),
        in_specs=[pl.BlockSpec(memory_space=pl.ANY)] * 8,
        out_specs=(vmem, vmem),
        scratch_shapes=[
            pltpu.VMEM(pair_exchange.shape, BF16),
            pltpu.VMEM(conduction.shape, BF16),
            pltpu.VMEM(valence.shape, BF16),
            pltpu.VMEM((1, LANES), F32),
            pltpu.VMEM((screening.shape[0], LANES), F32),
            pltpu.VMEM(vectors.shape, BF16),
            pltpu.SMEM(energies.shape, F32),
            pltpu.SMEM(k_coords.shape, jnp.int32),
            pltpu.VMEM((rows, 32, LANES), BF16),
            pltpu.VMEM((2, unit, LANES), F32),
            dma((8,)),
            pltpu.VMEM((cols, rows, 32, LANES), BF16),
            pltpu.VMEM((rows, nk, nb, LANES), BF16),
            pltpu.VMEM((batch, rows * 16), BF16),
            pltpu.VMEM((batch, rows * 16), BF16),
            pltpu.VMEM((LANES, nc * LANES), BF16),
            pltpu.VMEM((batch, kb * nvec), BF16),
            pltpu.VMEM((batch, batch), BF16),
            pltpu.VMEM((2 * points, count * 8), BF16),
            pltpu.VMEM((2 * LANES, LANES), BF16),
            pltpu.VMEM((cols, batch, LANES), BF16),
            pltpu.VMEM((cols, batch, LANES), F32),
            pltpu.VMEM((points, nvec, LANES), F32),
            pltpu.VMEM((cols, rows * 8, LANES), BF16),
            pltpu.VMEM((kb, points, LANES), F32),
            pltpu.VMEM((cols, nvec, LANES), F32),
            pltpu.VMEM((nc, rows, unit, nvec), F32),
            pltpu.VMEM((rows, unit, LANES), F32),
            pltpu.VMEM((rows, unit, LANES), F32),
            pltpu.VMEM((count, nvec // nc, LANES), F32),
            dma((cols, rows)), dma((cols, rows)),
            dma((rows,)), dma((rows,)),
            dma((cols,)), dma((cols,)),
            dma((count,)), dma((count,)),
            dma((rows,)), dma((rows,)),
        ],
        compiler_params=pltpu.CompilerParams(collective_id=0, has_side_effects=True),
    )(pair_exchange, conduction, valence, coulomb.reshape(1, planes), screening, vectors, energies, k_coords)


highest = lax.Precision.HIGHEST


def pair_factors(conduction, valence):
    count, valence_count, plane_count = valence.shape
    joined = (
        valence.astype(jnp.float32)[:, :, None, :] * conduction.astype(jnp.float32)[:, None, :, :]
    )
    return joined.reshape(count, valence_count * conduction.shape[1], plane_count).astype(
        jnp.bfloat16
    )


def transfer_index(rows_at, cols_at, mesh_cols):
    delta_first = jnp.mod(rows_at[:, None, 0] - cols_at[None, :, 0], MX)
    delta_second = jnp.mod(rows_at[:, None, 1] - cols_at[None, :, 1], mesh_cols)
    fold_first = jnp.minimum(delta_first, MX - delta_first)
    fold_second = jnp.minimum(delta_second, mesh_cols - delta_second)
    return (fold_first * (mesh_cols // 2 + 1) + fold_second).astype(jnp.int32)


def on_device(pair_exchange, conduction, valence, coulomb, screening, energies, vectors, k_coords):
    local_count, band_count, plane_count = pair_exchange.shape
    vector_count = vectors.shape[1] // band_count
    row_count = lax.axis_size("row")
    col_count = lax.axis_size("col")
    total_count = local_count * row_count * col_count
    mesh_cols = total_count // MX
    moving = vectors.reshape(local_count, band_count, vector_count)
    partial_density = jnp.einsum(
        "ktg,ktn->gn", pair_exchange, moving, preferred_element_type=jnp.float32
    )
    density = lax.psum(partial_density, ("row", "col"))
    block_size = 128
    sweeps = plane_count // block_size
    col_cond, col_val, col_vec, col_at = (
        lax.all_gather(conduction, "row", axis=0, tiled=True),
        lax.all_gather(valence, "row", axis=0, tiled=True),
        lax.all_gather(vectors, "row", axis=0, tiled=True),
        lax.all_gather(k_coords, "row", axis=0, tiled=True),
    )
    row_cond, row_val, row_at = (
        lax.all_gather(conduction, "col", axis=0, tiled=True),
        lax.all_gather(valence, "col", axis=0, tiled=True),
        lax.all_gather(k_coords, "col", axis=0, tiled=True),
    )
    row_pairs = pair_factors(row_cond, row_val)
    col_pairs = pair_factors(col_cond, col_val)
    indices = transfer_index(row_at, col_at, mesh_cols)
    col_moving = col_vec.reshape(-1, band_count, vector_count)

    def square_sweep(sweep_index, running):
        anchor = sweep_index * block_size
        coupling = jnp.take(
            lax.dynamic_slice_in_dim(screening, anchor, block_size, 1), indices, axis=0
        )
        row_block = lax.dynamic_slice_in_dim(row_pairs, anchor, block_size, 2)
        col_block = lax.dynamic_slice_in_dim(col_pairs, anchor, block_size, 2)
        col_proj = jnp.einsum(
            "ktg,ktn->kng", col_block, col_moving, preferred_element_type=jnp.float32
        )
        potential = jnp.einsum("ijg,jng->ing", coupling, col_proj, precision=highest)
        return running + jnp.einsum(
            "ktg,kng->ktn", row_block.astype(jnp.float32), potential, precision=highest
        )

    forward = lax.fori_loop(
        0,
        sweeps,
        square_sweep,
        jnp.zeros((row_pairs.shape[0], band_count, vector_count), jnp.float32),
    )
    owned = lax.psum_scatter(
        forward.reshape(col_count, local_count, band_count, vector_count),
        "col",
        scatter_dimension=0,
        tiled=True,
    )[0]
    moving_wide = moving.astype(jnp.float32)
    exchange_term = jnp.einsum(
        "ktg,gn->ktn", pair_exchange.astype(jnp.float32) * coulomb, density, precision=highest
    )
    applied = (
        energies[:, :, None] * moving_wide
        + 2.0 / (total_count * band_count) * exchange_term
        - owned / total_count
    )
    gram = jnp.einsum("ktm,ktn->mn", moving_wide, applied, precision=highest)
    alpha = lax.psum(gram, ("row", "col")) / (total_count * band_count)
    residual = applied - jnp.einsum("ktm,mn->ktn", moving_wide, alpha, precision=highest)
    return (residual.reshape(local_count, band_count * vector_count), alpha)


def fits(args, mesh):
    pair_exchange, conduction, valence, _, screening, _, vectors, _ = args
    rows, cols = mesh.shape["row"], mesh.shape["col"]
    points, nb, planes = pair_exchange.shape
    nk = points // (rows * cols)
    nv, nc = valence.shape[1], conduction.shape[1]
    nvec = vectors.shape[1] // nb
    return (
        planes == rows * LANES and nc * nvec == LANES and nk * nv == 8 and nk * (nv + nc) == 16
        and nk == 2 and nvec // nc == 8 and rows % 2 == 0 and screening.shape[0] <= LANES
        and points <= LANES
    )


def solution(mesh):
    in_specs = (
        P(("row", "col"), None, None),
        P(("row", "col"), None, None),
        P(("row", "col"), None, None),
        P(),
        P(),
        P(("row", "col"), None),
        P(("row", "col"), None),
        P(("row", "col"), None),
    )
    out_specs = (P(("row", "col"), None), P())

    def run(*args):
        body = fast_on_device if fits(args, mesh) else on_device
        return jax.shard_map(
            body, mesh=mesh, in_specs=in_specs, out_specs=out_specs, check_vma=False
        )(*args)

    return run
```

```python
import functools

import jax
import jax.numpy as jnp
from jax import lax
from jax.experimental import pallas as pl
from jax.experimental.pallas import tpu as pltpu
from jax.sharding import PartitionSpec as P

MX = 32
LANES = 128
MESH = pl.DeviceIdType.MESH
F32 = jnp.float32
BF16 = jnp.bfloat16


def split_pair(value):
    high = value.astype(BF16)
    return high, (value - high.astype(F32)).astype(BF16)


def dot(a, b, contract):
    return lax.dot_general(a, b, ((contract[0:1], contract[1:2]), ((), ())), preferred_element_type=F32)


def iota(shape, axis):
    return lax.broadcasted_iota(jnp.int32, shape, axis)


def one_hot(condition):
    return jnp.where(condition, 1.0, 0.0).astype(BF16)


def kernel(
    dims, px_hbm, cond_hbm, val_hbm, coulomb_hbm, screening_hbm, vec_hbm, energy_hbm, place_hbm,
    out_ref, alpha_ref,
    px_ref, cond_ref, val_ref, coulomb_ref, screening_ref, vec_ref, energy_ref, place_ref, msg_ref, wide_ref, load_sem,
    slots, px_slots, sel_v, sel_c, tile_m, block_m, perm, sel_k, screen, tiled, pairs, proj, coords, coupling,
    dens_slots, partial, out_send, out_slots, gram_slots,
    in_send, in_recv, px_send, px_recv, dens_send, dens_recv, gram_send, gram_recv, o_send, o_recv,
):
    rows, cols, nk, nv, nc, nvec, total, mesh_cols = dims
    row, col = lax.axis_index("row"), lax.axis_index("col")
    me = row * cols + col
    count = rows * cols
    kb = rows * nk
    nb = nv * nc
    unit = nk * nv
    per = kb * nv
    batch = per * nc

    def other(step):
        peer = lax.rem(me + step, count)
        return peer // cols, lax.rem(peer, cols)

    barrier = pltpu.get_barrier_semaphore()

    for step in range(1, rows):
        pl.semaphore_signal(barrier, inc=1, device_id=(lax.rem(row + step, rows), col), device_id_type=MESH)
    for step in range(1, cols):
        pl.semaphore_signal(barrier, inc=1, device_id=(row, lax.rem(col + step, cols)), device_id_type=MESH)

    mine = pl.ds(pl.multiple_of(row * LANES, LANES), LANES)
    loads = [
        pltpu.make_async_copy(src, dst, load_sem.at[at])
        for at, (src, dst) in enumerate((
            (val_hbm, val_ref), (cond_hbm, cond_ref), (vec_hbm, vec_ref), (place_hbm, place_ref), (energy_hbm, energy_ref), (px_hbm, px_ref),
            (screening_hbm.at[:, mine], screening_ref), (coulomb_hbm.at[:, mine], coulomb_ref)))
    ]
    for load in loads:
        load.start()
    for load in loads[:5]:
        load.wait()
    row8 = iota((8, LANES), 0)
    lane8 = iota((8, LANES), 1)
    spots = jnp.zeros((8, LANES), F32)
    for axis in range(2):
        for k in range(nk):
            spots = jnp.where(row8 == axis * nk + k, place_ref[k, axis].astype(F32), spots)
    energy = jnp.zeros((8, LANES), F32)
    for k in range(nk):
        for t in range(nb):
            energy = jnp.where((row8 == k * nv + t // nc) & (lane8 // nvec == t % nc), energy_ref[k, t], energy)
    vec = vec_ref[...].astype(F32)
    packed_own = jnp.concatenate(
        [vec[k:k + 1, j * LANES:(j + 1) * LANES] for k in range(nk) for j in range(nv)], axis=0)
    wide_ref[0] = packed_own
    wide_ref[1] = energy * packed_own
    message = jnp.concatenate(
        [ref[k].astype(F32) for k in range(nk) for ref in (val_ref, cond_ref)], axis=0).astype(BF16)
    extra = jnp.concatenate([packed_own, spots], axis=0).astype(BF16)
    for r in range(rows):
        msg_ref[r, 0:16] = message[:, r * LANES:(r + 1) * LANES]
        msg_ref[r, 16:32] = extra

    at = iota((batch, rows * 16), 0)
    to = iota((batch, rows * 16), 1)
    base = (at // unit) % rows * 16 + (at // nv) % nk * 8
    sel_v[...] = one_hot(to == base + at % nv)
    sel_c[...] = one_hot(to == base + nv + at // per)
    at = iota((LANES, nc * LANES), 0)
    to = iota((LANES, nc * LANES), 1)
    tile_m[...] = one_hot((at // nvec == to // LANES) & (at % nvec == to % nvec))
    at = iota((batch, kb * nvec), 0)
    to = iota((batch, kb * nvec), 1)
    block_m[...] = one_hot((at // nv) % kb == to // nvec)
    at = iota((batch, rows * nk * nb), 0)
    to = iota((batch, rows * nk * nb), 1)
    perm[...] = one_hot(to == (at // nv) % kb * nb + at % nv * nc + at // per)
    at = iota((2 * cols * kb, count * 8), 0)
    to = iota((2 * cols * kb, count * 8), 1)
    point = at % (cols * kb)
    sel_k[...] = one_hot(to == point // nk * 8 + at // (cols * kb) * nk + point % nk)
    for load in loads[5:]:
        load.wait()
    slots[col, row] = msg_ref[row]
    high, low = split_pair(jnp.concatenate(
        [screening_ref[...], jnp.zeros((LANES - screening_ref.shape[0], LANES), F32)], axis=0))
    screen[0:LANES] = high
    screen[LANES:2 * LANES] = low

    pl.semaphore_wait(barrier, rows + cols - 2)

    def in_copy(step):
        pr = lax.rem(row + step, rows)
        return pltpu.make_async_remote_copy(
            src_ref=msg_ref.at[pr, 0:28], dst_ref=slots.at[col, row, 0:28],
            send_sem=in_send.at[col, pr], recv_sem=in_recv.at[col, row],
            device_id=(pr, col), device_id_type=MESH)

    def across(step):
        far = lax.rem(col // 2 + step // 2, cols // 2)
        return far * 2 + lax.rem(lax.rem(col, 2) + lax.rem(step, 2), 2)

    def relay_copy(r, step):
        pc = across(step)
        return pltpu.make_async_remote_copy(
            src_ref=slots.at[col, r, 0:28], dst_ref=slots.at[col, r, 0:28],
            send_sem=in_send.at[pc, r], recv_sem=in_recv.at[col, r],
            device_id=(row, pc), device_id_type=MESH)

    def px_copy(step):
        pr = lax.rem(row + step, rows)
        return pltpu.make_async_remote_copy(
            src_ref=px_ref.at[:, :, pl.ds(pl.multiple_of(pr * LANES, LANES), LANES)], dst_ref=px_slots.at[row],
            send_sem=px_send.at[pr], recv_sem=px_recv.at[row],
            device_id=(pr, col), device_id_type=MESH)

    def dens_copy(step):
        pc = lax.rem(col + step, cols)
        return pltpu.make_async_remote_copy(
            src_ref=dens_slots.at[col], dst_ref=dens_slots.at[col],
            send_sem=dens_send.at[pc], recv_sem=dens_recv.at[col],
            device_id=(row, pc), device_id_type=MESH)

    def gram_copy(step):
        pr, pc = other(step)
        return pltpu.make_async_remote_copy(
            src_ref=gram_slots.at[me], dst_ref=gram_slots.at[me],
            send_sem=gram_send.at[pr * cols + pc], recv_sem=gram_recv.at[me],
            device_id=(pr, pc), device_id_type=MESH)

    def o_copy(step):
        pr = lax.rem(row + step, rows)
        return pltpu.make_async_remote_copy(
            src_ref=out_send.at[pr], dst_ref=out_slots.at[row],
            send_sem=o_send.at[pr], recv_sem=o_recv.at[row],
            device_id=(pr, col), device_id_type=MESH)

    def start_all(copy, end):
        def body(step, carry):
            copy(step).start()
            return carry
        lax.fori_loop(1, end, body, 0)

    def landed(ref, sem):
        pltpu.make_async_copy(ref, ref, sem).wait()

    start_all(in_copy, rows)
    start_all(px_copy, rows)
    px_slots[row] = px_ref[:, :, mine]

    def relay(d, carry):
        r = lax.rem(row + d, rows)
        landed(slots.at[col, r, 0:28], in_recv.at[col, r])
        for step in range(1, cols):
            relay_copy(r, step).start()
        return carry

    for step in range(1, cols):
        relay_copy(row, step).start()
    lax.fori_loop(1, rows, relay, 0)

    def take_batch(which):
        got = slots[which]
        factors = got[:, 0:16, :].reshape(rows * 16, LANES)
        rest = got[:, 16:32, :].astype(F32)
        packed = rest[:, 0:8, :].reshape(per, LANES).astype(BF16)
        spots_in = rest[:, 8:16, :].reshape(rows * 8, LANES)
        coords[which] = jnp.where(iota(spots_in.shape, 0) % 8 < 4, spots_in, 0.0).astype(BF16)
        wide = dot(packed, tile_m[...], (1, 0)).astype(BF16)
        stacked = jnp.concatenate([wide[:, s * LANES:(s + 1) * LANES] for s in range(nc)], axis=0)
        tiled[which] = stacked
        joined = (dot(sel_v[...], factors, (1, 0)) * dot(sel_c[...], factors, (1, 0))).astype(BF16)
        pairs[which] = joined.astype(F32)
        spread = jnp.concatenate([stacked] * (kb * nvec // LANES), axis=1) * block_m[...]
        projected = dot(spread, joined, (0, 0))
        proj[pl.ds(which * kb, kb)] = projected.reshape(kb, nvec, LANES)

    take_batch(col)

    def px_wait(step, carry):
        r = lax.rem(row + step, rows)
        landed(px_slots.at[r], px_recv.at[r])
        return carry

    lax.fori_loop(1, rows, px_wait, 0)
    px = dot(perm[...], px_slots[...].reshape(rows * nk * nb, LANES), (1, 0)).astype(BF16)
    own_x = tiled[col][:, 0:nvec]
    dens_slots[col] = dot(own_x, px, (0, 0))
    start_all(dens_copy, cols)

    def rest_batches(step, carry):
        c = across(step)

        def wait_one(r, inner):
            landed(slots.at[c, r, 0:28], in_recv.at[c, r])
            return inner

        lax.fori_loop(0, rows, wait_one, 0)
        take_batch(c)
        return carry

    lax.fori_loop(1, cols, rest_batches, 0)

    place = dot(sel_k[...], coords[...].reshape(count * 8, LANES), (1, 0))
    points = cols * kb
    first, second = place[0:points], place[points:2 * points]
    lane = iota((points, LANES), 1).astype(F32)
    coupling[0, 0:points] = first
    coupling[1, 0:points] = second
    start = pl.multiple_of(col * kb, kb)
    own_first = coupling[0, pl.ds(start, kb), :]
    own_second = coupling[1, pl.ds(start, kb), :]
    hots = []
    for i in range(kb):
        da = jnp.abs(own_first[i:i + 1] - first)
        db = jnp.abs(own_second[i:i + 1] - second)
        q = jnp.minimum(da, MX - da) * (mesh_cols // 2 + 1) + jnp.minimum(db, mesh_cols - db)
        hots.append(one_hot(q == lane))
    for i in range(kb):
        coupling[i] = dot(jnp.concatenate([hots[i], hots[i]], axis=1), screen[...], (1, 0))

    def dens_wait(step, carry):
        c = lax.rem(col + step, cols)
        landed(dens_slots.at[c], dens_recv.at[c])
        return carry

    lax.fori_loop(1, cols, dens_wait, 0)
    density = dens_slots[0]
    for c in range(1, cols):
        density = density + dens_slots[c]
    high, low = split_pair(density * coulomb_ref[...] * (2.0 / (total * nb)))
    partial[...] = (dot(px, high, (1, 1)) + dot(px, low, (1, 1))).reshape(nc, rows, unit, nvec)

    wide_own = wide_ref[1]
    for s in range(nc):
        partial[s, row] = partial[s, row] + wide_own[:, s * nvec:(s + 1) * nvec]

    group = 4
    row_k = (iota((nc * unit, LANES), 0) // nv) % nk
    potentials = []
    for block in range(kb // group):
        def gather(j, sums):
            term = proj[j]
            return tuple(
                sums[u] + coupling[block * group + u, pl.ds(j, 1), :] * term for u in range(group))
        potentials += list(lax.fori_loop(
            0, points, gather, tuple(jnp.zeros((nvec, LANES), F32) for _ in range(group)), unroll=8))
    for r in range(rows):
        mine_pairs = pairs[col].reshape(nc, rows, unit, LANES)[:, r].reshape(nc * unit, LANES)
        left = jnp.concatenate(
            [jnp.where(row_k == k, mine_pairs, 0.0) for k in range(nk)], axis=1).astype(BF16)
        high, low = split_pair(jnp.concatenate([potentials[r * nk + k] for k in range(nk)], axis=1))
        direct = dot(left, high, (1, 1)) + dot(left, low, (1, 1))
        for s in range(nc):
            partial[s, r] = partial[s, r] - direct[s * unit:(s + 1) * unit] * (1.0 / total)

    whole = partial[...]
    packed = jnp.concatenate([whole[s].reshape(per, nvec) for s in range(nc)], axis=1)
    out_send[...] = packed.reshape(rows, unit, LANES)
    start_all(o_copy, rows)
    high, low = split_pair(whole.reshape(batch, nvec))
    gram = dot(own_x, high, (0, 0)) + dot(own_x, low, (0, 0))
    step = nvec // nc
    gram_slots[me] = jnp.concatenate([gram[s * step:(s + 1) * step] for s in range(nc)], axis=1)
    start_all(gram_copy, count)

    def o_wait(d, acc):
        r = lax.rem(row + d, rows)
        landed(out_slots.at[r], o_recv.at[r])
        return acc + out_slots[r]

    applied = lax.fori_loop(1, rows, o_wait, out_send[row])

    def gram_wait(d, carry):
        p = lax.rem(me + d, count)
        landed(gram_slots.at[p], gram_recv.at[p])
        return carry

    lax.fori_loop(1, count, gram_wait, 0)
    sums = jnp.sum(gram_slots[...], axis=0) * (1.0 / (total * nb))
    alpha = jnp.concatenate([sums[:, s * nvec:(s + 1) * nvec] for s in range(nc)], axis=0)
    alpha_ref[...] = alpha
    own = wide_ref[0]
    own_rows = jnp.concatenate([own[:, s * nvec:(s + 1) * nvec] for s in range(nc)], axis=0).astype(BF16)
    high, low = split_pair(alpha)
    taken = dot(own_rows, high, (1, 0)) + dot(own_rows, low, (1, 0))
    residual = applied - jnp.concatenate([taken[s * unit:(s + 1) * unit] for s in range(nc)], axis=1)
    for j in range(nv):
        out_ref[:, j * LANES:(j + 1) * LANES] = jnp.concatenate(
            [residual[k * nv + j:k * nv + j + 1] for k in range(nk)], axis=0)

    def drain(copy, end):
        def body(d, carry):
            copy(d).wait_send()
            return carry
        lax.fori_loop(1, end, body, 0)

    drain(in_copy, rows)

    def drain_relay(r, carry):
        for step in range(1, cols):
            relay_copy(r, step).wait_send()
        return carry

    lax.fori_loop(0, rows, drain_relay, 0)
    drain(px_copy, rows)
    drain(dens_copy, cols)
    drain(o_copy, rows)
    drain(gram_copy, count)


def fast_on_device(pair_exchange, conduction, valence, coulomb, screening, energies, vectors, k_coords):
    nk, nb, planes = pair_exchange.shape
    nv, nc = valence.shape[1], conduction.shape[1]
    nvec = vectors.shape[1] // nb
    rows, cols = lax.axis_size("row"), lax.axis_size("col")
    count = rows * cols
    total = nk * count
    unit = nk * nv
    kb = rows * nk
    batch = kb * nb
    vmem = pl.BlockSpec(memory_space=pltpu.VMEM)
    dma = pltpu.SemaphoreType.DMA
    points = cols * kb
    return pl.pallas_call(
        functools.partial(kernel, (rows, cols, nk, nv, nc, nvec, total, total // MX)),
        out_shape=(
            pltpu.VMEM((nk, nb * nvec), F32),
            pltpu.VMEM((nvec, nvec), F32),
        ),
        in_specs=[pl.BlockSpec(memory_space=pl.ANY)] * 8,
        out_specs=(vmem, vmem),
        scratch_shapes=[
            pltpu.VMEM(pair_exchange.shape, BF16),
            pltpu.VMEM(conduction.shape, BF16),
            pltpu.VMEM(valence.shape, BF16),
            pltpu.VMEM((1, LANES), F32),
            pltpu.VMEM((screening.shape[0], LANES), F32),
            pltpu.VMEM(vectors.shape, BF16),
            pltpu.SMEM(energies.shape, F32),
            pltpu.SMEM(k_coords.shape, jnp.int32),
            pltpu.VMEM((rows, 32, LANES), BF16),
            pltpu.VMEM((2, unit, LANES), F32),
            dma((8,)),
            pltpu.VMEM((cols, rows, 32, LANES), BF16),
            pltpu.VMEM((rows, nk, nb, LANES), BF16),
            pltpu.VMEM((batch, rows * 16), BF16),
            pltpu.VMEM((batch, rows * 16), BF16),
            pltpu.VMEM((LANES, nc * LANES), BF16),
            pltpu.VMEM((batch, kb * nvec), BF16),
            pltpu.VMEM((batch, batch), BF16),
            pltpu.VMEM((2 * points, count * 8), BF16),
            pltpu.VMEM((2 * LANES, LANES), BF16),
            pltpu.VMEM((cols, batch, LANES), BF16),
            pltpu.VMEM((cols, batch, LANES), F32),
            pltpu.VMEM((points, nvec, LANES), F32),
            pltpu.VMEM((cols, rows * 8, LANES), BF16),
            pltpu.VMEM((kb, points, LANES), F32),
            pltpu.VMEM((cols, nvec, LANES), F32),
            pltpu.VMEM((nc, rows, unit, nvec), F32),
            pltpu.VMEM((rows, unit, LANES), F32),
            pltpu.VMEM((rows, unit, LANES), F32),
            pltpu.VMEM((count, nvec // nc, LANES), F32),
            dma((cols, rows)), dma((cols, rows)),
            dma((rows,)), dma((rows,)),
            dma((cols,)), dma((cols,)),
            dma((count,)), dma((count,)),
            dma((rows,)), dma((rows,)),
        ],
        compiler_params=pltpu.CompilerParams(collective_id=0, has_side_effects=True),
    )(pair_exchange, conduction, valence, coulomb.reshape(1, planes), screening, vectors, energies, k_coords)


highest = lax.Precision.HIGHEST


def pair_factors(conduction, valence):
    count, valence_count, plane_count = valence.shape
    joined = (
        valence.astype(jnp.float32)[:, :, None, :] * conduction.astype(jnp.float32)[:, None, :, :]
    )
    return joined.reshape(count, valence_count * conduction.shape[1], plane_count).astype(
        jnp.bfloat16
    )


def transfer_index(rows_at, cols_at, mesh_cols):
    delta_first = jnp.mod(rows_at[:, None, 0] - cols_at[None, :, 0], MX)
    delta_second = jnp.mod(rows_at[:, None, 1] - cols_at[None, :, 1], mesh_cols)
    fold_first = jnp.minimum(delta_first, MX - delta_first)
    fold_second = jnp.minimum(delta_second, mesh_cols - delta_second)
    return (fold_first * (mesh_cols // 2 + 1) + fold_second).astype(jnp.int32)


def on_device(pair_exchange, conduction, valence, coulomb, screening, energies, vectors, k_coords):
    local_count, band_count, plane_count = pair_exchange.shape
    vector_count = vectors.shape[1] // band_count
    row_count = lax.axis_size("row")
    col_count = lax.axis_size("col")
    total_count = local_count * row_count * col_count
    mesh_cols = total_count // MX
    moving = vectors.reshape(local_count, band_count, vector_count)
    partial_density = jnp.einsum(
        "ktg,ktn->gn", pair_exchange, moving, preferred_element_type=jnp.float32
    )
    density = lax.psum(partial_density, ("row", "col"))
    block_size = 128
    sweeps = plane_count // block_size
    col_cond, col_val, col_vec, col_at = (
        lax.all_gather(conduction, "row", axis=0, tiled=True),
        lax.all_gather(valence, "row", axis=0, tiled=True),
        lax.all_gather(vectors, "row", axis=0, tiled=True),
        lax.all_gather(k_coords, "row", axis=0, tiled=True),
    )
    row_cond, row_val, row_at = (
        lax.all_gather(conduction, "col", axis=0, tiled=True),
        lax.all_gather(valence, "col", axis=0, tiled=True),
        lax.all_gather(k_coords, "col", axis=0, tiled=True),
    )
    row_pairs = pair_factors(row_cond, row_val)
    col_pairs = pair_factors(col_cond, col_val)
    indices = transfer_index(row_at, col_at, mesh_cols)
    col_moving = col_vec.reshape(-1, band_count, vector_count)

    def square_sweep(sweep_index, running):
        anchor = sweep_index * block_size
        coupling = jnp.take(
            lax.dynamic_slice_in_dim(screening, anchor, block_size, 1), indices, axis=0
        )
        row_block = lax.dynamic_slice_in_dim(row_pairs, anchor, block_size, 2)
        col_block = lax.dynamic_slice_in_dim(col_pairs, anchor, block_size, 2)
        col_proj = jnp.einsum(
            "ktg,ktn->kng", col_block, col_moving, preferred_element_type=jnp.float32
        )
        potential = jnp.einsum("ijg,jng->ing", coupling, col_proj, precision=highest)
        return running + jnp.einsum(
            "ktg,kng->ktn", row_block.astype(jnp.float32), potential, precision=highest
        )

    forward = lax.fori_loop(
        0,
        sweeps,
        square_sweep,
        jnp.zeros((row_pairs.shape[0], band_count, vector_count), jnp.float32),
    )
    owned = lax.psum_scatter(
        forward.reshape(col_count, local_count, band_count, vector_count),
        "col",
        scatter_dimension=0,
        tiled=True,
    )[0]
    moving_wide = moving.astype(jnp.float32)
    exchange_term = jnp.einsum(
        "ktg,gn->ktn", pair_exchange.astype(jnp.float32) * coulomb, density, precision=highest
    )
    applied = (
        energies[:, :, None] * moving_wide
        + 2.0 / (total_count * band_count) * exchange_term
        - owned / total_count
    )
    gram = jnp.einsum("ktm,ktn->mn", moving_wide, applied, precision=highest)
    alpha = lax.psum(gram, ("row", "col")) / (total_count * band_count)
    residual = applied - jnp.einsum("ktm,mn->ktn", moving_wide, alpha, precision=highest)
    return (residual.reshape(local_count, band_count * vector_count), alpha)


def fits(args, mesh):
    pair_exchange, conduction, valence, _, screening, _, vectors, _ = args
    rows, cols = mesh.shape["row"], mesh.shape["col"]
    points, nb, planes = pair_exchange.shape
    nk = points // (rows * cols)
    nv, nc = valence.shape[1], conduction.shape[1]
    nvec = vectors.shape[1] // nb
    return (
        planes == rows * LANES and nc * nvec == LANES and nk * nv == 8 and nk * (nv + nc) == 16
        and nk == 2 and nvec // nc == 8 and rows % 2 == 0 and cols % 2 == 0 and screening.shape[0] <= LANES
        and points <= LANES
    )


def solution(mesh):
    in_specs = (
        P(("row", "col"), None, None),
        P(("row", "col"), None, None),
        P(("row", "col"), None, None),
        P(),
        P(),
        P(("row", "col"), None),
        P(("row", "col"), None),
        P(("row", "col"), None),
    )
    out_specs = (P(("row", "col"), None), P())

    def run(*args):
        body = fast_on_device if fits(args, mesh) else on_device
        return jax.shard_map(
            body, mesh=mesh, in_specs=in_specs, out_specs=out_specs, check_vma=False
        )(*args)

    return run
```
